128 devices in a mesh: data: 1, dap2: 16 (over z, y), dap: 8 (over x, core).
Axes of the slice: x: 4, y: 4, z: 4, core: 2. Of those that a mesh axis runs over, the one named last changes fastest.
Arguments:
- pair_rep: float32 [1024, 1024, 128], P(('data', 'dap2', 'dap'))
- pair_mask: int32 [1024, 1024], P(('data', 'dap2', 'dap'))
- norm_gain: bfloat16 [2, 128], replicated
- norm_bias: bfloat16 [2, 128], replicated
- w_proj: bfloat16 [2, 128, 512], replicated
- w_gate: bfloat16 [2, 128, 128], replicated
- post_gain: bfloat16 [2, 128], replicated
- post_bias: bfloat16 [2, 128], replicated
- w_out: bfloat16 [2, 128, 128], replicated
Outputs:
- output: float32 [1024, 1024, 128], P(('data', 'dap2', 'dap'))
All inputs are finite; a program needn't handle non-finite values.
Results may differ from the reference program's by a relative error of at most 0.00102608.
Values are sent between devices in bfloat16 or wider.
A program may use at most 1 GiB of HBM per device.

```python
import jax
import jax.numpy as jnp
from jax import lax

N = 1024
CZ = 128
C = 128
ROW_BLOCKS = 8
BLOCK_ROWS = N // ROW_BLOCKS
NORM_EPS = 1e-5


def setup_inputs(seed: int = 0, part: int = 0) -> dict:
    part_key = jax.random.fold_in(jax.random.key(seed), part)
    pair_key, length_key = jax.random.split(part_key, 2)
    pair_rep = jax.random.normal(pair_key, (N, N, CZ), jnp.float32)
    length = jax.random.randint(length_key, (), N - N // 8, N - N // 16 + 1)
    valid_rows = jnp.arange(N) < length
    pair_mask = (valid_rows[:, None] & valid_rows[None, :]).astype(jnp.int32)
    param_keys = jax.random.split(jax.random.key(seed + 1), 7)
    norm_gain = 1.0 + 0.3 * jax.random.normal(param_keys[0], (2, CZ), jnp.float32)
    norm_bias = 0.3 * jax.random.normal(param_keys[1], (2, CZ), jnp.float32)
    w_proj = jax.random.normal(param_keys[2], (2, CZ, 4 * C), jnp.float32) * CZ ** -0.5
    w_gate = jax.random.normal(param_keys[3], (2, CZ, CZ), jnp.float32) * CZ ** -0.5
    post_gain = 1.0 + 0.3 * jax.random.normal(param_keys[4], (2, C), jnp.float32)
    post_bias = 0.3 * jax.random.normal(param_keys[5], (2, C), jnp.float32)
    w_out = jax.random.normal(param_keys[6], (2, C, CZ), jnp.float32) * (2.0 * C ** -0.5)
    return {
        'pair_rep': pair_rep,
        'pair_mask': pair_mask,
        'norm_gain': norm_gain.astype(jnp.bfloat16),
        'norm_bias': norm_bias.astype(jnp.bfloat16),
        'w_proj': w_proj.astype(jnp.bfloat16),
        'w_gate': w_gate.astype(jnp.bfloat16),
        'post_gain': post_gain.astype(jnp.bfloat16),
        'post_bias': post_bias.astype(jnp.bfloat16),
        'w_out': w_out.astype(jnp.bfloat16),
    }


def layer_norm(values, scale_vec, shift_vec, norm_axis):
    row_mean = jnp.mean(values, axis=norm_axis, keepdims=True)
    centered = values - row_mean
    row_var = jnp.mean(centered * centered, axis=norm_axis, keepdims=True)
    scaled = centered * lax.rsqrt(row_var + NORM_EPS)
    return (scaled * scale_vec.astype(jnp.float32) + shift_vec.astype(jnp.float32)).astype(jnp.bfloat16)


def gated_side(normed, w_pair, keep_blk):
    projected = jnp.dot(normed.reshape(-1, CZ), w_pair, preferred_element_type=jnp.float32)
    projected = projected.reshape(BLOCK_ROWS, N, 2 * C)
    return (keep_blk[..., None] * jax.nn.sigmoid(projected[..., C:]) * projected[..., :C]).astype(jnp.bfloat16)


def outgoing_mix(pair_in):
    return jnp.dot(pair_in[0], pair_in[1].T, preferred_element_type=jnp.float32)


def incoming_mix(pair_in):
    return jnp.dot(pair_in[0].T, pair_in[1], preferred_element_type=jnp.float32)


def tri_update(pair_rep, keep_mask, norm_gain, norm_bias, w_proj, w_gate, post_gain, post_bias, w_out, mix_fn):
    pair_blocks = pair_rep.reshape(ROW_BLOCKS, BLOCK_ROWS, N, CZ)
    keep_blocks = keep_mask.reshape(ROW_BLOCKS, BLOCK_ROWS, N)

    def project(block_in):
        pair_blk, keep_blk = block_in
        normed = layer_norm(pair_blk, norm_gain, norm_bias, -1)
        return (gated_side(normed, w_proj[:, :2 * C], keep_blk),
                gated_side(normed, w_proj[:, 2 * C:], keep_blk))

    side_a, side_b = lax.map(project, (pair_blocks, keep_blocks))
    chan_a = jnp.moveaxis(side_a.reshape(N, N, C), 2, 0)
    chan_b = jnp.moveaxis(side_b.reshape(N, N, C), 2, 0)
    mixed_sum = lax.map(mix_fn, (chan_a, chan_b))
    mixed_blocks = jnp.moveaxis(mixed_sum.reshape(C, ROW_BLOCKS, BLOCK_ROWS, N), 1, 0)

    def finish(block_in):
        pair_blk, mixed_blk = block_in
        normed = layer_norm(pair_blk, norm_gain, norm_bias, -1)
        post_norm = layer_norm(mixed_blk, post_gain[:, None, None], post_bias[:, None, None], 0)
        update = jnp.dot(jnp.moveaxis(post_norm, 0, -1).reshape(-1, C), w_out, preferred_element_type=jnp.float32)
        gate_pre = jnp.dot(normed.reshape(-1, CZ), w_gate, preferred_element_type=jnp.float32)
        gated_out = jax.nn.sigmoid(gate_pre) * update
        return pair_blk + gated_out.reshape(BLOCK_ROWS, N, CZ)

    return lax.map(finish, (pair_blocks, mixed_blocks)).reshape(N, N, CZ)


def reference(pair_rep, pair_mask, norm_gain, norm_bias, w_proj, w_gate, post_gain, post_bias, w_out):
    keep_mask = pair_mask.astype(jnp.float32)
    pair_mid = tri_update(pair_rep, keep_mask, norm_gain[0], norm_bias[0], w_proj[0], w_gate[0],
                          post_gain[0], post_bias[0], w_out[0], outgoing_mix)
    return tri_update(pair_mid, keep_mask, norm_gain[1], norm_bias[1], w_proj[1], w_gate[1],
                      post_gain[1], post_bias[1], w_out[1], incoming_mix)
```

```python
import jax
import jax.numpy as jnp
from jax import lax
from jax.experimental import pallas as pl
from jax.experimental.pallas import tpu as pltpu
from jax.sharding import PartitionSpec as P

NORM_EPS = 1e-5
ROW_SPEC = P(('data', 'dap2', 'dap'), None, None)
MASK_SPEC = P(('data', 'dap2', 'dap'), None)

N = 1024
C = 128
ROWS = 8
LANES = 128
BLOCKS = N // LANES
CHUNKS = 4
PER = BLOCKS // CHUNKS


def norm_t(values, gain, bias):
    mean = jnp.sum(values, axis=0, keepdims=True) * (1.0 / C)
    centered = values - mean
    var = jnp.sum(centered * centered, axis=0, keepdims=True) * (1.0 / C)
    return (centered * lax.rsqrt(var + NORM_EPS) * gain + bias).astype(jnp.bfloat16)


def body(z_ref, mask_ref, wproj_ref, wgate_ref, wout_ref, vec_ref, out_ref,
         y_ref, g_ref, yn_ref, stage_ref, sab_ref, rab0_ref, rab1_ref, sx_ref, rx0_ref, rx1_ref, a_ref, b_ref,
         ssem, rsem):
    d2 = lax.axis_index('dap2')
    d1 = lax.axis_index('dap')
    me = d2 * 8 + d1
    mz, my, mx, mc = lax.div(d2, 4), lax.rem(d2, 4), lax.div(d1, 2), lax.rem(d1, 2)
    lines = [lax.rem(mx + dx, 4) * 2 + lax.rem(mc + dc, 2) for dx in range(4) for dc in range(2)]

    def everyone(fn):
        @pl.loop(0, 16)
        def _(o):
            t2 = lax.rem(mz + lax.div(o, 4), 4) * 4 + lax.rem(my + lax.rem(o, 4), 4)
            for n in range(1, 8):
                fn(t2, lines[n])

            @pl.when(o != 0)
            def _():
                fn(t2, lines[0])

    barrier = pltpu.get_barrier_semaphore()
    everyone(lambda t2, t1: pl.semaphore_signal(
        barrier, 1, device_id={'dap2': t2, 'dap': t1}, device_id_type=pl.DeviceIdType.MESH))

    def send(src_of, dst, kind, q):
        everyone(lambda t2, t1: pltpu.make_async_remote_copy(
            src_of(t2 * 8 + t1), dst, ssem.at[kind, q], rsem.at[kind, q],
            device_id={'dap2': t2, 'dap': t1}, device_id_type=pl.DeviceIdType.MESH).start())

    def arrival(ref, kind, q):
        return pltpu.make_async_remote_copy(ref, ref, ssem.at[kind, q], rsem.at[kind, q],
                                            device_id={'dap2': d2, 'dap': d1},
                                            device_id_type=pl.DeviceIdType.MESH)

    def lanes_of(kb):
        return pl.ds(pl.multiple_of(kb * LANES, LANES), LANES)

    def project(s, y, r, lanes):
        yn = norm_t(y, vec_ref[s, 0], vec_ref[s, 1])
        yn_ref[r, :, lanes] = yn
        keep = mask_ref[r, :, lanes].astype(jnp.float32)
        for side in range(2):
            p = jnp.dot(wproj_ref[s, 2 * C * side:2 * C * (side + 1), :], yn, preferred_element_type=jnp.float32)
            stage_ref[side, pl.ds(r, C, stride=ROWS), :] = keep * jax.nn.sigmoid(p[C:]) * p[:C]

    def pack(kb):
        sides = [stage_ref[side].reshape(C, ROWS, LANES) for side in range(2)]
        sab_ref[kb] = jnp.concatenate(sides, axis=1).astype(jnp.bfloat16)

    def gates(s):
        @pl.loop(0, BLOCKS)
        def _(kb):
            @pl.loop(0, ROWS)
            def _(r):
                pre = jnp.dot(wgate_ref[s], yn_ref[r, :, lanes_of(kb)], preferred_element_type=jnp.float32)
                g_ref[r, :, lanes_of(kb)] = jax.nn.sigmoid(pre)

    def send_sides(q, rab_ref, kind):
        blocks = pl.ds(q * PER, PER)
        send(lambda t: sab_ref.at[blocks, t], rab_ref.at[blocks, me], kind, q)
        rab_ref[blocks, me] = sab_ref[blocks, me]

    def send_mix(q, rx_ref, kind):
        blocks = pl.ds(q * PER, PER)
        send(lambda t: sx_ref.at[blocks, pl.ds(pl.multiple_of(t * ROWS, ROWS), ROWS)],
             rx_ref.at[blocks, pl.ds(pl.multiple_of(me * ROWS, ROWS), ROWS)], kind, q)
        own = pl.ds(pl.multiple_of(me * ROWS, ROWS), ROWS)
        rx_ref[blocks, own] = sx_ref[blocks, own]

    def wait_sides(q, rab_ref, kind):
        arrival(rab_ref.at[pl.ds(q * PER, PER), pl.ds(0, C - 1)], kind, q).wait_recv()

    def wait_mix(q, rx_ref, kind):
        arrival(rx_ref.at[pl.ds(q * PER, PER), pl.ds(0, N - ROWS)], kind, q).wait_recv()

    def drain(kind, q):
        if kind in (0, 2):
            arrival(sab_ref.at[pl.ds(q * PER, PER), pl.ds(0, C - 1)], kind, q).wait_send()
        else:
            arrival(sx_ref.at[pl.ds(q * PER, PER), pl.ds(0, N - ROWS)], kind, q).wait_send()

    def update_of(s, rx_ref, kb, r):
        lanes = lanes_of(kb)
        xn = norm_t(rx_ref[kb, pl.ds(r, C, stride=ROWS), :], vec_ref[s, 2], vec_ref[s, 3])
        upd = jnp.dot(wout_ref[s], xn, preferred_element_type=jnp.float32)
        return y_ref[r, :, lanes] + g_ref[r, :, lanes] * upd

    @pl.loop(0, CHUNKS)
    def _(q):
        @pl.loop(q * PER, (q + 1) * PER)
        def _(kb):
            @pl.loop(0, ROWS)
            def _(r):
                y = z_ref[r, lanes_of(kb), :].T
                y_ref[r, :, lanes_of(kb)] = y
                project(0, y, r, lanes_of(kb))
            pack(kb)

        @pl.when(q == 0)
        def _():
            pl.semaphore_wait(barrier, 127)
        send_sides(q, rab0_ref, 0)
    gates(0)

    @pl.loop(0, CHUNKS)
    def _(q):
        wait_sides(q, rab0_ref, 0)

        @pl.loop(q * PER, (q + 1) * PER)
        def _(kb):
            both = rab0_ref[kb].astype(jnp.float32)
            a_ref[:, lanes_of(kb)] = both[:, :ROWS].reshape(N, LANES).astype(jnp.bfloat16)
            b_ref[:, lanes_of(kb)] = both[:, ROWS:].reshape(N, LANES).astype(jnp.bfloat16)

    @pl.loop(0, CHUNKS)
    def _(q):
        @pl.loop(q * PER, (q + 1) * PER)
        def _(jb):
            rows = b_ref[pl.ds(pl.multiple_of(jb * LANES, LANES), LANES), :]
            sx_ref[jb] = lax.dot_general(a_ref[...], rows, (((1,), (1,)), ((), ())),
                                         preferred_element_type=jnp.float32)
        send_mix(q, rx0_ref, 1)

    @pl.loop(0, CHUNKS)
    def _(q):
        drain(0, q)
    @pl.loop(0, CHUNKS)
    def _(q):
        wait_mix(q, rx0_ref, 1)

        @pl.loop(q * PER, (q + 1) * PER)
        def _(kb):
            @pl.loop(0, ROWS)
            def _(r):
                y = update_of(0, rx0_ref, kb, r)
                y_ref[r, :, lanes_of(kb)] = y
                project(1, y, r, lanes_of(kb))
            pack(kb)
        send_sides(q, rab1_ref, 2)
    gates(1)

    @pl.loop(0, CHUNKS)
    def _(q):
        drain(1, q)
    @pl.loop(0, CHUNKS)
    def _(q):
        wait_sides(q, rab1_ref, 2)

        @pl.loop(q * PER, (q + 1) * PER)
        def _(kb):
            both = rab1_ref[kb].astype(jnp.float32)
            a_ref[pl.ds(pl.multiple_of(kb * LANES, LANES), LANES), :] = (
                both[:, :ROWS].reshape(N, LANES).T.astype(jnp.bfloat16))
            b_ref[:, lanes_of(kb)] = both[:, ROWS:].reshape(N, LANES).astype(jnp.bfloat16)

    @pl.loop(0, CHUNKS)
    def _(q):
        @pl.loop(q * PER, (q + 1) * PER)
        def _(jb):
            sx_ref[jb] = jnp.dot(a_ref[...], b_ref[:, lanes_of(jb)], preferred_element_type=jnp.float32)
        send_mix(q, rx1_ref, 3)

    @pl.loop(0, CHUNKS)
    def _(q):
        wait_mix(q, rx1_ref, 3)

        @pl.loop(q * PER, (q + 1) * PER)
        def _(kb):
            @pl.loop(0, ROWS)
            def _(r):
                out_ref[r, lanes_of(kb), :] = update_of(1, rx1_ref, kb, r).T

    @pl.loop(0, CHUNKS)
    def _(q):
        drain(2, q)
        drain(3, q)


def solution(mesh):
    def local_step(pair_rows, mask_rows, norm_gain, norm_bias, w_proj, w_gate, post_gain, post_bias, w_out):
        vecs = jnp.stack([norm_gain, norm_bias, post_gain, post_bias], axis=1).astype(jnp.float32)
        vecs = jnp.broadcast_to(vecs[..., None], vecs.shape + (LANES,))
        turned = [jnp.swapaxes(w, 1, 2) for w in (w_proj, w_gate, w_out)]
        vmem = pl.BlockSpec(memory_space=pltpu.VMEM)
        sides = pltpu.VMEM((BLOCKS, C, 2 * ROWS, LANES), jnp.bfloat16)
        mix = pltpu.VMEM((BLOCKS, N, LANES), jnp.float32)
        rows = pltpu.VMEM((ROWS, C, N), jnp.float32)
        square = pltpu.VMEM((N, N), jnp.bfloat16)
        return pl.pallas_call(
            body,
            name='triangle_pair',
            out_shape=jax.ShapeDtypeStruct(pair_rows.shape, jnp.float32),
            in_specs=[vmem] * 6,
            out_specs=vmem,
            scratch_shapes=[rows, rows, pltpu.VMEM((ROWS, C, N), jnp.bfloat16),
                            pltpu.VMEM((2, N, LANES), jnp.float32),
                            sides, sides, sides, mix, mix, mix, square, square,
                            pltpu.SemaphoreType.DMA((4, CHUNKS)), pltpu.SemaphoreType.DMA((4, CHUNKS))],
            compiler_params=pltpu.CompilerParams(collective_id=0, has_side_effects=True,
                                                 vmem_limit_bytes=66_000_000),
        )(pair_rows, mask_rows[:, None], *turned, vecs)

    replicated = P()
    return jax.shard_map(local_step, mesh=mesh,
                         in_specs=(ROW_SPEC, MASK_SPEC) + (replicated,) * 7,
                         out_specs=ROW_SPEC, check_vma=False)
```

```python
import jax
import jax.numpy as jnp
from jax import lax
from jax.experimental import pallas as pl
from jax.experimental.pallas import tpu as pltpu
from jax.sharding import PartitionSpec as P

NORM_EPS = 1e-5
ROW_SPEC = P(('data', 'dap2', 'dap'), None, None)
MASK_SPEC = P(('data', 'dap2', 'dap'), None)

N = 1024
C = 128
ROWS = 8
LANES = 128
BLOCKS = N // LANES
CHUNKS = 4
PER = BLOCKS // CHUNKS
WIDE = PER * LANES
UNROLL = 2


def partner_offsets():
    kinds = {}
    for z in range(4):
        for y in range(4):
            for x in range(4):
                kinds.setdefault(tuple(sorted(min(v, 4 - v) for v in (z, y, x))), []).append((z, y, x))
    offsets = []
    for kind in sorted(kinds, key=lambda k: (-sum(k), k)):
        group = []
        for first in kinds[kind]:
            for turn in range(3):
                turned = first[turn:] + first[:turn]
                for entry in (turned, tuple((4 - v) % 4 for v in turned)):
                    if entry not in group:
                        group.append(entry)
        for core in range(2):
            offsets += [entry + (core,) for entry in group if entry + (core,) != (0, 0, 0, 0)]
    return offsets


OFFSETS = partner_offsets()


def norm_t(values, gain, bias):
    mean = jnp.sum(values, axis=0, keepdims=True) * (1.0 / C)
    centered = values - mean
    var = jnp.sum(centered * centered, axis=0, keepdims=True) * (1.0 / C)
    return (centered * lax.rsqrt(var + NORM_EPS) * gain + bias).astype(jnp.bfloat16)


def scoped(name, fn, *args):
    with jax.named_scope(name):
        return fn(*args)


def body(z_hbm, mask_ref, ngain_ref, nbias_ref, wproj_in, wgate_in, pgain_ref, pbias_ref, wout_in, out_hbm,
         z_ref, keep_ref, wproj_ref, wgate_ref, wout_ref, vec_ref,
         y_ref, g_ref, yn_ref, stage_ref, sab_ref, rab0_ref, rab1_ref, sx_ref, rx0_ref, rx1_ref, a_ref, b_ref,
         ssem, rsem, zsem, osem):
    def z_copy(q):
        cols = pl.ds(pl.multiple_of(q * WIDE, WIDE), WIDE)
        return pltpu.make_async_copy(z_hbm.at[:, cols], z_ref.at[:, cols], zsem.at[q])

    def out_copy(q):
        cols = pl.ds(pl.multiple_of(q * WIDE, WIDE), WIDE)
        return pltpu.make_async_copy(z_ref.at[:, cols], out_hbm.at[:, cols], osem.at[q])

    for q in range(CHUNKS):
        z_copy(q).start()

    d2 = lax.axis_index('dap2')
    d1 = lax.axis_index('dap')
    me = d2 * 8 + d1
    mz, my, mx, mc = lax.div(d2, 4), lax.rem(d2, 4), lax.div(d1, 2), lax.rem(d1, 2)
    lines = {(dx, dc): lax.rem(mx + dx, 4) * 2 + lax.rem(mc + dc, 2) for dx in range(4) for dc in range(2)}
    planes = {(dz, dy): lax.rem(mz + dz, 4) * 4 + lax.rem(my + dy, 4) for dz in range(4) for dy in range(4)}

    def everyone(fn):
        for dz, dy, dx, dc in OFFSETS:
            fn(planes[dz, dy], lines[dx, dc])

    barrier = pltpu.get_barrier_semaphore()
    everyone(lambda t2, t1: pl.semaphore_signal(
        barrier, 1, device_id={'dap2': t2, 'dap': t1}, device_id_type=pl.DeviceIdType.MESH))

    def send(src_of, dst, kind, q):
        everyone(lambda t2, t1: pltpu.make_async_remote_copy(
            src_of(t2 * 8 + t1), dst, ssem.at[kind, q], rsem.at[kind, q],
            device_id={'dap2': t2, 'dap': t1}, device_id_type=pl.DeviceIdType.MESH).start())

    def arrival(ref, kind, q):
        return pltpu.make_async_remote_copy(ref, ref, ssem.at[kind, q], rsem.at[kind, q],
                                            device_id={'dap2': d2, 'dap': d1},
                                            device_id_type=pl.DeviceIdType.MESH)

    def lanes_of(kb):
        return pl.ds(pl.multiple_of(kb * LANES, LANES), LANES)

    def wide_of(q):
        return pl.ds(pl.multiple_of(q * WIDE, WIDE), WIDE)

    def vec(s, n):
        return jnp.concatenate([vec_ref[s, n]] * PER, axis=1)

    def project(s, y, r, q):
        yn = norm_t(y, vec(s, 0), vec(s, 1))
        yn_ref[r, :, wide_of(q)] = yn
        keep = keep_ref[r, :, wide_of(q)]
        for side in range(2):
            p = jnp.dot(wproj_ref[s, 2 * C * side:2 * C * (side + 1), :], yn, preferred_element_type=jnp.float32)
            part = keep * jax.nn.sigmoid(p[C:]) * p[:C]
            for n in range(PER):
                stage_ref[side, n, pl.ds(r, C, stride=ROWS), :] = part[:, n * LANES:(n + 1) * LANES]

    def column(ref, s):
        return jnp.broadcast_to(ref[...].astype(jnp.float32)[s:s + 1], (C, LANES)).T

    def turn(ref, s, lo):
        return ref[s, :, lo:lo + C].astype(jnp.float32).T.astype(jnp.bfloat16)

    def set_up_norm(s):
        vec_ref[s, 0] = column(ngain_ref, s)
        vec_ref[s, 1] = column(nbias_ref, s)
        for n in range(4):
            wproj_ref[s, n * C:(n + 1) * C] = turn(wproj_in, s, n * C)

    def set_up_rest(s):
        vec_ref[s, 2] = column(pgain_ref, s)
        vec_ref[s, 3] = column(pbias_ref, s)
        wgate_ref[s] = turn(wgate_in, s, 0)
        wout_ref[s] = turn(wout_in, s, 0)

    def pack(q):
        for n in range(PER):
            sides = [stage_ref[side, n].reshape(C, ROWS, LANES) for side in range(2)]
            sab_ref[q * PER + n] = jnp.concatenate(sides, axis=1).astype(jnp.bfloat16)

    def gates(s):
        @pl.loop(0, CHUNKS)
        def _(q):
            @pl.loop(0, ROWS, unroll=2)
            def _(r):
                pre = jnp.dot(wgate_ref[s], yn_ref[r, :, wide_of(q)], preferred_element_type=jnp.float32)
                g_ref[r, :, wide_of(q)] = jax.nn.sigmoid(pre)

    def send_sides(q, rab_ref, kind):
        blocks = pl.ds(q * PER, PER)
        send(lambda t: sab_ref.at[blocks, t], rab_ref.at[blocks, me], kind, q)
        rab_ref[blocks, me] = sab_ref[blocks, me]

    def send_mix(q, rx_ref, kind):
        blocks = pl.ds(q * PER, PER)
        send(lambda t: sx_ref.at[blocks, pl.ds(pl.multiple_of(t * ROWS, ROWS), ROWS)],
             rx_ref.at[blocks, pl.ds(pl.multiple_of(me * ROWS, ROWS), ROWS)], kind, q)
        own = pl.ds(pl.multiple_of(me * ROWS, ROWS), ROWS)
        rx_ref[blocks, own] = sx_ref[blocks, own]

    def wait_sides(q, rab_ref, kind):
        arrival(rab_ref.at[pl.ds(q * PER, PER), pl.ds(0, C - 1)], kind, q).wait_recv()

    def wait_mix(q, rx_ref, kind):
        arrival(rx_ref.at[pl.ds(q * PER, PER), pl.ds(0, N - ROWS)], kind, q).wait_recv()

    def drain(kind, q):
        if kind in (0, 2):
            arrival(sab_ref.at[pl.ds(q * PER, PER), pl.ds(0, C - 1)], kind, q).wait_send()
        else:
            arrival(sx_ref.at[pl.ds(q * PER, PER), pl.ds(0, N - ROWS)], kind, q).wait_send()

    def update_of(s, rx_ref, q, r):
        x = jnp.concatenate([rx_ref[q * PER + n, pl.ds(r, C, stride=ROWS), :] for n in range(PER)], axis=1)
        xn = norm_t(x, vec(s, 2), vec(s, 3))
        upd = jnp.dot(wout_ref[s], xn, preferred_element_type=jnp.float32)
        return y_ref[r, :, wide_of(q)] + g_ref[r, :, wide_of(q)] * upd

    for r in range(ROWS):
        keep_ref[r] = mask_ref[r:r + 1, :].astype(jnp.float32)
    set_up_norm(0)

    @pl.loop(0, CHUNKS)
    def _(q):
        z_copy(q).wait()

        @pl.loop(0, ROWS, unroll=UNROLL)
        def _(r):
            y = z_ref[r, wide_of(q), :].T
            y_ref[r, :, wide_of(q)] = y
            project(0, y, r, q)
        pack(q)

        @pl.when(q == 0)
        def _():
            scoped('entry', pl.semaphore_wait, barrier, 127)
        scoped('send_s0', send_sides, q, rab0_ref, 0)
    set_up_rest(0)
    set_up_norm(1)
    set_up_rest(1)
    scoped('gates', gates, 0)

    @pl.loop(0, CHUNKS)
    def _(q):
        scoped('wait_s0', wait_sides, q, rab0_ref, 0)

        @pl.loop(q * PER, (q + 1) * PER)
        def _(kb):
            both = rab0_ref[kb].astype(jnp.float32)
            a_ref[:, lanes_of(kb)] = both[:, :ROWS].reshape(N, LANES).astype(jnp.bfloat16)
            b_ref[:, lanes_of(kb)] = both[:, ROWS:].reshape(N, LANES).astype(jnp.bfloat16)

    @pl.loop(0, CHUNKS)
    def _(q):
        @pl.loop(q * PER, (q + 1) * PER)
        def _(jb):
            rows = b_ref[pl.ds(pl.multiple_of(jb * LANES, LANES), LANES), :]
            sx_ref[jb] = lax.dot_general(a_ref[...], rows, (((1,), (1,)), ((), ())),
                                         preferred_element_type=jnp.float32)
        scoped('send_m0', send_mix, q, rx0_ref, 1)

    @pl.loop(0, CHUNKS)
    def _(q):
        drain(0, q)
    @pl.loop(0, CHUNKS)
    def _(q):
        scoped('wait_m0', wait_mix, q, rx0_ref, 1)

        @pl.loop(0, ROWS, unroll=UNROLL)
        def _(r):
            y = update_of(0, rx0_ref, q, r)
            y_ref[r, :, wide_of(q)] = y
            project(1, y, r, q)
        pack(q)
        scoped('send_s1', send_sides, q, rab1_ref, 2)
    scoped('gates', gates, 1)

    @pl.loop(0, CHUNKS)
    def _(q):
        drain(1, q)
    @pl.loop(0, CHUNKS)
    def _(q):
        scoped('wait_s1', wait_sides, q, rab1_ref, 2)

        @pl.loop(q * PER, (q + 1) * PER)
        def _(kb):
            both = rab1_ref[kb].astype(jnp.float32)
            a_ref[pl.ds(pl.multiple_of(kb * LANES, LANES), LANES), :] = (
                both[:, :ROWS].reshape(N, LANES).T.astype(jnp.bfloat16))
            b_ref[:, lanes_of(kb)] = both[:, ROWS:].reshape(N, LANES).astype(jnp.bfloat16)

    @pl.loop(0, CHUNKS)
    def _(q):
        @pl.loop(q * PER, (q + 1) * PER)
        def _(jb):
            sx_ref[jb] = jnp.dot(a_ref[...], b_ref[:, lanes_of(jb)], preferred_element_type=jnp.float32)
        scoped('send_m1', send_mix, q, rx1_ref, 3)

    @pl.loop(0, CHUNKS)
    def _(q):
        scoped('wait_m1', wait_mix, q, rx1_ref, 3)

        @pl.loop(0, ROWS, unroll=UNROLL)
        def _(r):
            z_ref[r, wide_of(q), :] = update_of(1, rx1_ref, q, r).T
        out_copy(q).start()

    @pl.loop(0, CHUNKS)
    def _(q):
        drain(2, q)
        drain(3, q)
        out_copy(q).wait()


def solution(mesh):
    def local_step(*args):
        vmem = pl.BlockSpec(memory_space=pltpu.VMEM)
        hbm = pl.BlockSpec(memory_space=pl.ANY)
        f32, bf16 = jnp.float32, jnp.bfloat16
        sides = pltpu.VMEM((BLOCKS, C, 2 * ROWS, LANES), bf16)
        mix = pltpu.VMEM((BLOCKS, N, LANES), f32)
        rows = pltpu.VMEM((ROWS, C, N), f32)
        square = pltpu.VMEM((N, N), bf16)
        exchange = pltpu.SemaphoreType.DMA((4, CHUNKS))
        chunk = pltpu.SemaphoreType.DMA((CHUNKS,))
        return pl.pallas_call(
            body,
            name='triangle_pair',
            out_shape=jax.ShapeDtypeStruct((ROWS, N, C), f32),
            in_specs=[hbm] + [vmem] * 8,
            out_specs=hbm,
            scratch_shapes=[pltpu.VMEM((ROWS, N, C), f32), pltpu.VMEM((ROWS, 1, N), f32),
                            pltpu.VMEM((2, 4 * C, C), bf16), pltpu.VMEM((2, C, C), bf16),
                            pltpu.VMEM((2, C, C), bf16), pltpu.VMEM((2, 4, C, LANES), f32),
                            rows, rows, pltpu.VMEM((ROWS, C, N), bf16), pltpu.VMEM((2, PER, N, LANES), f32),
                            sides, sides, sides, mix, mix, mix, square, square,
                            exchange, exchange, chunk, chunk],
            compiler_params=pltpu.CompilerParams(collective_id=0, has_side_effects=True,
                                                 vmem_limit_bytes=66_000_000),
        )(*args)

    replicated = P()
    return jax.shard_map(local_step, mesh=mesh,
                         in_specs=(ROW_SPEC, MASK_SPEC) + (replicated,) * 7,
                         out_specs=ROW_SPEC, check_vma=False)
```

```python
import random

import jax
import jax.numpy as jnp
from jax import lax
from jax.experimental import pallas as pl
from jax.experimental.pallas import tpu as pltpu
from jax.sharding import PartitionSpec as P

NORM_EPS = 1e-5
ROW_SPEC = P(('data', 'dap2', 'dap'), None, None)
MASK_SPEC = P(('data', 'dap2', 'dap'), None)

N = 1024
C = 128
ROWS = 8
LANES = 128
BLOCKS = N // LANES
CHUNKS = 8
PER = BLOCKS // CHUNKS
WIDE = PER * LANES
UNROLL = 2


def partner_offsets():
    offsets = [(z, y, x, c) for z in range(4) for y in range(4) for x in range(4) for c in range(2)][1:]
    random.Random(0).shuffle(offsets)
    return offsets


OFFSETS = partner_offsets()


def norm_t(values, gain, bias):
    mean = jnp.sum(values, axis=0, keepdims=True) * (1.0 / C)
    centered = values - mean
    var = jnp.sum(centered * centered, axis=0, keepdims=True) * (1.0 / C)
    return (centered * lax.rsqrt(var + NORM_EPS) * gain + bias).astype(jnp.bfloat16)


def scoped(name, fn, *args):
    with jax.named_scope(name):
        return fn(*args)


def body(z_hbm, mask_ref, ngain_ref, nbias_ref, wproj_in, wgate_in, pgain_ref, pbias_ref, wout_in, out_hbm,
         z_ref, keep_ref, wproj_ref, wgate_ref, wout_ref, vec_ref,
         y_ref, g_ref, yn_ref, stage_ref, sab_ref, rab0_ref, rab1_ref, sx_ref, rx0_ref, rx1_ref, a_ref, b_ref,
         ssem, rsem, zsem, osem):
    def z_copy(q):
        cols = pl.ds(pl.multiple_of(q * WIDE, WIDE), WIDE)
        return pltpu.make_async_copy(z_hbm.at[:, cols], z_ref.at[:, cols], zsem.at[q])

    def out_copy(q):
        cols = pl.ds(pl.multiple_of(q * WIDE, WIDE), WIDE)
        return pltpu.make_async_copy(z_ref.at[:, cols], out_hbm.at[:, cols], osem.at[q])

    for q in range(CHUNKS):
        z_copy(q).start()

    d2 = lax.axis_index('dap2')
    d1 = lax.axis_index('dap')
    me = d2 * 8 + d1
    mz, my, mx, mc = lax.div(d2, 4), lax.rem(d2, 4), lax.div(d1, 2), lax.rem(d1, 2)
    lines = {(dx, dc): lax.rem(mx + dx, 4) * 2 + lax.rem(mc + dc, 2) for dx in range(4) for dc in range(2)}
    planes = {(dz, dy): lax.rem(mz + dz, 4) * 4 + lax.rem(my + dy, 4) for dz in range(4) for dy in range(4)}

    def everyone(fn):
        for dz, dy, dx, dc in OFFSETS:
            fn(planes[dz, dy], lines[dx, dc])

    barrier = pltpu.get_barrier_semaphore()
    everyone(lambda t2, t1: pl.semaphore_signal(
        barrier, 1, device_id={'dap2': t2, 'dap': t1}, device_id_type=pl.DeviceIdType.MESH))

    def send(src_of, dst, kind, q):
        everyone(lambda t2, t1: pltpu.make_async_remote_copy(
            src_of(t2 * 8 + t1), dst, ssem.at[kind, q], rsem.at[kind, q],
            device_id={'dap2': t2, 'dap': t1}, device_id_type=pl.DeviceIdType.MESH).start())

    def arrival(ref, kind, q):
        return pltpu.make_async_remote_copy(ref, ref, ssem.at[kind, q], rsem.at[kind, q],
                                            device_id={'dap2': d2, 'dap': d1},
                                            device_id_type=pl.DeviceIdType.MESH)

    def lanes_of(kb):
        return pl.ds(pl.multiple_of(kb * LANES, LANES), LANES)

    def wide_of(q):
        return pl.ds(pl.multiple_of(q * WIDE, WIDE), WIDE)

    def vec(s, n):
        return jnp.concatenate([vec_ref[s, n]] * PER, axis=1)

    def project(s, y, r, q):
        yn = norm_t(y, vec(s, 0), vec(s, 1))
        yn_ref[r, :, wide_of(q)] = yn
        keep = keep_ref[r, :, wide_of(q)]
        for side in range(2):
            p = jnp.dot(wproj_ref[s, 2 * C * side:2 * C * (side + 1), :], yn, preferred_element_type=jnp.float32)
            part = keep * jax.nn.sigmoid(p[C:]) * p[:C]
            for n in range(PER):
                stage_ref[side, n, pl.ds(r, C, stride=ROWS), :] = part[:, n * LANES:(n + 1) * LANES]

    def column(ref, s):
        return jnp.broadcast_to(ref[...].astype(jnp.float32)[s:s + 1], (C, LANES)).T

    def turn(ref, s, lo):
        return ref[s, :, lo:lo + C].astype(jnp.float32).T.astype(jnp.bfloat16)

    def set_up_norm(s):
        vec_ref[s, 0] = column(ngain_ref, s)
        vec_ref[s, 1] = column(nbias_ref, s)
        for n in range(4):
            wproj_ref[s, n * C:(n + 1) * C] = turn(wproj_in, s, n * C)

    def set_up_rest(s):
        vec_ref[s, 2] = column(pgain_ref, s)
        vec_ref[s, 3] = column(pbias_ref, s)
        wgate_ref[s] = turn(wgate_in, s, 0)
        wout_ref[s] = turn(wout_in, s, 0)

    def pack(q):
        for n in range(PER):
            sides = [stage_ref[side, n].reshape(C, ROWS, LANES) for side in range(2)]
            sab_ref[q * PER + n] = jnp.concatenate(sides, axis=1).astype(jnp.bfloat16)

    def gates(s):
        @pl.loop(0, CHUNKS)
        def _(q):
            @pl.loop(0, ROWS, unroll=2)
            def _(r):
                pre = jnp.dot(wgate_ref[s], yn_ref[r, :, wide_of(q)], preferred_element_type=jnp.float32)
                g_ref[r, :, wide_of(q)] = jax.nn.sigmoid(pre)

    def send_sides(q, rab_ref, kind):
        blocks = pl.ds(q * PER, PER)
        send(lambda t: sab_ref.at[blocks, t], rab_ref.at[blocks, me], kind, q)
        rab_ref[blocks, me] = sab_ref[blocks, me]

    def send_mix(q, rx_ref, kind):
        blocks = pl.ds(q * PER, PER)
        send(lambda t: sx_ref.at[blocks, pl.ds(pl.multiple_of(t * ROWS, ROWS), ROWS)],
             rx_ref.at[blocks, pl.ds(pl.multiple_of(me * ROWS, ROWS), ROWS)], kind, q)
        own = pl.ds(pl.multiple_of(me * ROWS, ROWS), ROWS)
        rx_ref[blocks, own] = sx_ref[blocks, own]

    def wait_sides(q, rab_ref, kind):
        arrival(rab_ref.at[pl.ds(q * PER, PER), pl.ds(0, C - 1)], kind, q).wait_recv()

    def wait_mix(q, rx_ref, kind):
        arrival(rx_ref.at[pl.ds(q * PER, PER), pl.ds(0, N - ROWS)], kind, q).wait_recv()

    def drain(kind, q):
        if kind in (0, 2):
            arrival(sab_ref.at[pl.ds(q * PER, PER), pl.ds(0, C - 1)], kind, q).wait_send()
        else:
            arrival(sx_ref.at[pl.ds(q * PER, PER), pl.ds(0, N - ROWS)], kind, q).wait_send()

    def update_of(s, rx_ref, q, r):
        x = jnp.concatenate([rx_ref[q * PER + n, pl.ds(r, C, stride=ROWS), :] for n in range(PER)], axis=1)
        xn = norm_t(x, vec(s, 2), vec(s, 3))
        upd = jnp.dot(wout_ref[s], xn, preferred_element_type=jnp.float32)
        return y_ref[r, :, wide_of(q)] + g_ref[r, :, wide_of(q)] * upd

    for r in range(ROWS):
        keep_ref[r] = mask_ref[r:r + 1, :].astype(jnp.float32)
    set_up_norm(0)

    @pl.loop(0, CHUNKS)
    def _(q):
        z_copy(q).wait()

        @pl.loop(0, ROWS, unroll=UNROLL)
        def _(r):
            y = z_ref[r, wide_of(q), :].T
            y_ref[r, :, wide_of(q)] = y
            project(0, y, r, q)
        pack(q)

        @pl.when(q == 0)
        def _():
            scoped('entry', pl.semaphore_wait, barrier, 127)
        scoped('send_s0', send_sides, q, rab0_ref, 0)
    set_up_rest(0)
    set_up_norm(1)
    set_up_rest(1)
    scoped('gates', gates, 0)

    @pl.loop(0, CHUNKS)
    def _(q):
        scoped('wait_s0', wait_sides, q, rab0_ref, 0)

        @pl.loop(q * PER, (q + 1) * PER)
        def _(kb):
            both = rab0_ref[kb].astype(jnp.float32)
            a_ref[:, lanes_of(kb)] = both[:, :ROWS].reshape(N, LANES).astype(jnp.bfloat16)
            b_ref[:, lanes_of(kb)] = both[:, ROWS:].reshape(N, LANES).astype(jnp.bfloat16)

    @pl.loop(0, CHUNKS)
    def _(q):
        @pl.loop(q * PER, (q + 1) * PER)
        def _(jb):
            rows = b_ref[pl.ds(pl.multiple_of(jb * LANES, LANES), LANES), :]
            sx_ref[jb] = lax.dot_general(a_ref[...], rows, (((1,), (1,)), ((), ())),
                                         preferred_element_type=jnp.float32)
        scoped('send_m0', send_mix, q, rx0_ref, 1)

    @pl.loop(0, CHUNKS)
    def _(q):
        drain(0, q)
    @pl.loop(0, CHUNKS)
    def _(q):
        scoped('wait_m0', wait_mix, q, rx0_ref, 1)

        @pl.loop(0, ROWS, unroll=UNROLL)
        def _(r):
            y = update_of(0, rx0_ref, q, r)
            y_ref[r, :, wide_of(q)] = y
            project(1, y, r, q)
        pack(q)
        scoped('send_s1', send_sides, q, rab1_ref, 2)
    scoped('gates', gates, 1)

    @pl.loop(0, CHUNKS)
    def _(q):
        drain(1, q)
    @pl.loop(0, CHUNKS)
    def _(q):
        scoped('wait_s1', wait_sides, q, rab1_ref, 2)

        @pl.loop(q * PER, (q + 1) * PER)
        def _(kb):
            both = rab1_ref[kb].astype(jnp.float32)
            a_ref[pl.ds(pl.multiple_of(kb * LANES, LANES), LANES), :] = (
                both[:, :ROWS].reshape(N, LANES).T.astype(jnp.bfloat16))
            b_ref[:, lanes_of(kb)] = both[:, ROWS:].reshape(N, LANES).astype(jnp.bfloat16)

    @pl.loop(0, CHUNKS)
    def _(q):
        @pl.loop(q * PER, (q + 1) * PER)
        def _(jb):
            sx_ref[jb] = jnp.dot(a_ref[...], b_ref[:, lanes_of(jb)], preferred_element_type=jnp.float32)
        scoped('send_m1', send_mix, q, rx1_ref, 3)

    @pl.loop(0, CHUNKS)
    def _(q):
        scoped('wait_m1', wait_mix, q, rx1_ref, 3)

        @pl.loop(0, ROWS, unroll=UNROLL)
        def _(r):
            z_ref[r, wide_of(q), :] = update_of(1, rx1_ref, q, r).T
        out_copy(q).start()

    @pl.loop(0, CHUNKS)
    def _(q):
        drain(2, q)
        drain(3, q)
        out_copy(q).wait()


def solution(mesh):
    def local_step(*args):
        vmem = pl.BlockSpec(memory_space=pltpu.VMEM)
        hbm = pl.BlockSpec(memory_space=pl.ANY)
        f32, bf16 = jnp.float32, jnp.bfloat16
        sides = pltpu.VMEM((BLOCKS, C, 2 * ROWS, LANES), bf16)
        mix = pltpu.VMEM((BLOCKS, N, LANES), f32)
        rows = pltpu.VMEM((ROWS, C, N), f32)
        square = pltpu.VMEM((N, N), bf16)
        exchange = pltpu.SemaphoreType.DMA((4, CHUNKS))
        chunk = pltpu.SemaphoreType.DMA((CHUNKS,))
        return pl.pallas_call(
            body,
            name='triangle_pair',
            out_shape=jax.ShapeDtypeStruct((ROWS, N, C), f32),
            in_specs=[hbm] + [vmem] * 8,
            out_specs=hbm,
            scratch_shapes=[pltpu.VMEM((ROWS, N, C), f32), pltpu.VMEM((ROWS, 1, N), f32),
                            pltpu.VMEM((2, 4 * C, C), bf16), pltpu.VMEM((2, C, C), bf16),
                            pltpu.VMEM((2, C, C), bf16), pltpu.VMEM((2, 4, C, LANES), f32),
                            rows, rows, pltpu.VMEM((ROWS, C, N), bf16), pltpu.VMEM((2, PER, N, LANES), f32),
                            sides, sides, sides, mix, mix, mix, square, square,
                            exchange, exchange, chunk, chunk],
            compiler_params=pltpu.CompilerParams(collective_id=0, has_side_effects=True,
                                                 vmem_limit_bytes=66_000_000),
        )(*args)

    replicated = P()
    return jax.shard_map(local_step, mesh=mesh,
                         in_specs=(ROW_SPEC, MASK_SPEC) + (replicated,) * 7,
                         out_specs=ROW_SPEC, check_vma=False)
```
